32 devices in a mesh: pb: 4 (over z), freq: 4 (over y, core), ga: 2 (over x).
Axes of the slice: x: 2, y: 2, z: 4, core: 2. Of those that a mesh axis runs over, the one named last changes fastest.
Arguments:
- densities: bfloat16 [4, 2, 256, 4096], P('pb', None, ('freq', 'ga')), may hold values from -0.5 to 0.5
- screened: bfloat16 [4, 4, 2, 4096, 4096], P('pb', 'freq', None, 'ga'), may hold values from -0.09375 to 0.09375
- energies: float32 [16, 256], replicated, may hold values from -2.5 to 2.5
- occupied: int32 [16], replicated, may hold values from 64 to 192
- kmq: int32 [4], replicated, may hold values from 0 to 15
- offsets: int32 [4], replicated, may hold values from -16 to 15
- weights: float32 [4], replicated, may hold values from 0.5 to 2
Outputs:
- sigma: float32 [2, 1, 64], P(None, None, ('pb', 'freq'))
The draws below stay inside these ranges and needn't reach their ends.
All inputs are finite; a program needn't handle non-finite values.
Results may differ from the reference program's by a relative error of at most 0.0003.
Values may be sent and summed in bfloat16 or wider, within the bound.
A program may use at most 64 MiB of HBM per device.

```python
import math
import jax
import jax.numpy as jnp
from jax import lax

G = 4096
NB = 256
NS = 1
Q = 4
NKP = 16
NW = 4
NOUT = 64
K = 256


def place_ends(result, stream_key, least, high):
    longest = result.shape.index(max(result.shape))
    spots = []
    for shift in (0, 1):
        where = [jax.random.randint(jax.random.fold_in(stream_key, axis), (), 0, length) for axis, length in enumerate(result.shape)]
        where[longest] = (where[longest] + shift) % result.shape[longest]
        spots.append(tuple(where))
    return result.at[spots[0]].set(least).at[spots[1]].set(high)


def block_scale(rng, shape, split, least, top_value):
    def one(dim, blocks):
        steps = jax.random.uniform(jax.random.fold_in(jax.random.fold_in(rng, 6), dim), (blocks,), jnp.float32, least / len(split), top_value / len(split))
        return jnp.repeat(jnp.exp(steps), shape[dim] // blocks).reshape((-1,) + (1,) * (len(shape) - dim - 1))

    factor_of = one(*split[0])
    for cut in split[1:]:
        factor_of = factor_of * one(*cut)
    return factor_of


def centred(key, shape, width, reach, pieces=(), kind=jnp.bfloat16):
    result = width * jax.random.normal(key, shape, jnp.float32)
    if pieces:
        result = result * block_scale(key, shape, pieces, -0.22, 0.18)
    return jnp.clip(result, -reach, reach).astype(kind)


def setup_inputs(seed: int = 0) -> dict:
    key_list = jax.random.split(jax.random.key(seed), 8)
    return {
        "densities": centred(key_list[0], (Q, 2, K, G), (0.7071 * G ** -0.25), 0.5, ((0, 4), (2, 8))),
        "screened": centred(key_list[1], (Q, NW, 2, G, G), G ** -0.5, 0.09375, ((0, 4), (1, 4), (3, 2))),
        "energies": jnp.clip(jax.random.uniform(key_list[2], (NKP, NB), jnp.float32, -2.5, 2.5), -2.5, 2.5),
        "occupied": place_ends(jax.random.randint(key_list[3], (NKP,), NB // 4, 3 * NB // 4 + 1), jax.random.fold_in(key_list[3], 1), NB // 4, (3 * NB // 4 + 1) - 1).astype(jnp.int32),
        "kmq": place_ends(jax.random.randint(key_list[4], (Q,), 0, NKP), jax.random.fold_in(key_list[4], 1), 0, NKP - 1).astype(jnp.int32),
        "offsets": place_ends(jax.random.randint(key_list[5], (NW,), 0 - NOUT // 4, NOUT // 4), jax.random.fold_in(key_list[5], 1), 0 - NOUT // 4, (NOUT // 4) - 1).astype(jnp.int32),
        "weights": jnp.clip(jnp.exp(jax.random.uniform(key_list[6], (NW,), jnp.float32, math.log(0.5), math.log(2.0))), 0.5, 2.0),
    }


broadening = 0.15


def green_parts(level_row, filled, freq_shift, omegas):
    bands = jnp.arange(level_row.shape[0], dtype=jnp.int32)
    pole_sign = jnp.where(bands < filled, -1.0, 1.0).astype(jnp.float32)
    real_part = omegas[None, :] - freq_shift - level_row[:, None]
    imag_part = broadening * pole_sign[:, None]
    denominator = real_part * real_part + imag_part * imag_part
    return real_part / denominator, -imag_part / denominator


def spectrum(pair_real, pair_imag, green_real, green_imag):
    exact = lax.Precision.HIGHEST
    real_out = jnp.dot(pair_real, green_real, precision=exact) - jnp.dot(pair_imag, green_imag, precision=exact)
    imag_out = jnp.dot(pair_real, green_imag, precision=exact) + jnp.dot(pair_imag, green_real, precision=exact)
    return real_out, imag_out


def pair_sums(density, screen):
    pair_rows = density.shape[1]
    basis_rows = screen.shape[1]
    product = lax.dot_general(density.reshape(2 * pair_rows, -1), screen.reshape(2 * basis_rows, -1),
                              (((1,), (1,)), ((), ())), preferred_element_type=jnp.float32)
    product = product.reshape(2, pair_rows, 2, basis_rows)
    real_x = product[0, :, 0] - product[1, :, 1]
    imag_x = product[0, :, 1] + product[1, :, 0]
    dense = density.astype(jnp.float32)
    real_sum = jnp.sum(dense[0] * real_x + dense[1] * imag_x, axis=1)
    imag_sum = jnp.sum(dense[0] * imag_x - dense[1] * real_x, axis=1)
    return real_sum, imag_sum


def reference(densities, screened, energies, occupied, kmq, offsets, weights):
    omegas = -2.0 + 4.0 * jnp.arange(NOUT, dtype=jnp.float32) / NOUT
    summed_real = jnp.zeros((NS, NOUT), jnp.float32)
    summed_imag = jnp.zeros((NS, NOUT), jnp.float32)
    for qpoint in range(Q):
        kpoint = kmq[qpoint]
        level_row = energies[kpoint]
        filled = occupied[kpoint]
        for frequency in range(NW):
            real_sum, imag_sum = pair_sums(densities[qpoint], screened[qpoint, frequency])
            weight_now = weights[frequency]
            real_sum = (weight_now * real_sum).reshape(NS, NB)
            imag_sum = (weight_now * imag_sum).reshape(NS, NB)
            freq_shift = 4.0 * offsets[frequency].astype(jnp.float32) / NOUT
            green_real, green_imag = green_parts(level_row, filled, freq_shift, omegas)
            real_out, imag_out = spectrum(real_sum, imag_sum, green_real, green_imag)
            summed_real = summed_real + real_out
            summed_imag = summed_imag + imag_out
    prefactor = 1.0 / (2.0 * math.pi * Q)
    return jnp.stack([-prefactor * summed_imag, prefactor * summed_real])
```

```python
import functools
import math

import jax
import jax.numpy as jnp
from jax import lax
from jax.experimental import pallas as pl
from jax.experimental.pallas import tpu as pltpu
from jax.sharding import PartitionSpec as P

MESH = pl.DeviceIdType.MESH
CHUNKS = 8
TILE = 512
AHEAD = 3

NB = 256
NS = 1
OUT_DEV = 4


broadening = 0.15


def from_behind(block, axis, distance):
    devices = range(lax.axis_size(axis))
    route = [((i - distance) % len(devices), i) for i in devices]
    return lax.ppermute(block, axis, route)


def green_parts(level_row, filled, freq_shift, omegas):
    bands = jnp.arange(level_row.shape[0], dtype=jnp.int32)
    pole_sign = jnp.where(bands < filled, -1.0, 1.0).astype(jnp.float32)
    real_part = omegas[None, :] - freq_shift - level_row[:, None]
    imag_part = broadening * pole_sign[:, None]
    denominator = real_part * real_part + imag_part * imag_part
    return (real_part / denominator, -imag_part / denominator)


def spectrum(pair_real, pair_imag, green_real, green_imag):
    exact = lax.Precision.HIGHEST
    real_out = jnp.dot(pair_real, green_real, precision=exact) - jnp.dot(
        pair_imag, green_imag, precision=exact
    )
    imag_out = jnp.dot(pair_real, green_imag, precision=exact) + jnp.dot(
        pair_imag, green_real, precision=exact
    )
    return jnp.stack([real_out, imag_out])


def panel_product(density_all, screen):
    pair_rows = density_all.shape[1]
    panel_rows = screen.shape[1]
    product = lax.dot_general(
        density_all.reshape(2 * pair_rows, -1),
        screen.reshape(2 * panel_rows, -1),
        (((1,), (1,)), ((), ())),
        preferred_element_type=jnp.float32,
    )
    product = product.reshape(2, pair_rows, 2, panel_rows)
    return (product[0, :, 0] - product[1, :, 1], product[0, :, 1] + product[1, :, 0])


def plain_body(densities, screened, energies, occupied, kmq, offsets, weights):
    qpoint = lax.axis_index("pb")
    my_freq = lax.axis_index("freq")
    my_panel = lax.axis_index("ga")
    count_pb = lax.axis_size("pb")
    count_freq = lax.axis_size("freq")
    screen = screened[0, 0]
    panel_width = screen.shape[1]
    local_block = densities[0]
    whole = lax.all_gather(local_block, ("freq", "ga"), axis=1, tiled=True)
    real_x, imag_x = panel_product(whole, screen)
    own_rows = lax.dynamic_slice_in_dim(whole, my_panel * panel_width, panel_width, 2)
    dense = own_rows.astype(jnp.float32)
    real_sum = jnp.sum(dense[0] * real_x + dense[1] * imag_x, axis=1)
    imag_sum = jnp.sum(dense[0] * imag_x - dense[1] * real_x, axis=1)
    pair_total = lax.psum(jnp.stack([real_sum, imag_sum]), "ga")
    weighted = (pair_total * weights[my_freq]).reshape(2, NS, NB)
    kpoint = kmq[qpoint]
    level_row = energies[kpoint]
    filled = occupied[kpoint]
    total_out = OUT_DEV * count_pb * count_freq
    index_grid = (jnp.arange(count_pb, dtype=jnp.int32)[:, None] * count_freq + my_freq) * OUT_DEV
    index_grid = (index_grid + jnp.arange(OUT_DEV, dtype=jnp.int32)[None, :]).reshape(-1)
    omegas = -2.0 + 4.0 * index_grid.astype(jnp.float32) / total_out
    summed = jnp.zeros((2, NS, count_pb * OUT_DEV), jnp.float32)
    passed = weighted
    for rotation in range(count_freq):
        anchor = (my_freq - rotation) % count_freq
        freq_shift = 4.0 * offsets[anchor].astype(jnp.float32) / total_out
        green_real, green_imag = green_parts(level_row, filled, freq_shift, omegas)
        summed = summed + spectrum(passed[0], passed[1], green_real, green_imag)
        if rotation + 1 < count_freq:
            passed = from_behind(passed, "freq", 1)
    local_part = lax.psum_scatter(summed, "pb", scatter_dimension=2, tiled=True)
    prefactor = 1.0 / (2.0 * math.pi * count_pb)
    return jnp.stack([-prefactor * local_part[1], prefactor * local_part[0]])


def fused_kernel(
    shape,
    dens_ref,
    screen_ref,
    energy_ref,
    filled_ref,
    kmq_ref,
    offset_ref,
    weight_ref,
    out_ref,
    blocks,
    panel,
    acc,
    green,
    plane_parts,
    pb_parts,
    own_sem,
    panel_sem,
    send_sem,
    recv_sem,
    plane_send,
    plane_recv,
    pb_send,
    pb_recv,
):
    count_pb, count_freq, count_ga, chunks, width, tile = shape
    group = count_freq * count_ga
    pair_rows = blocks.shape[3]
    pairs = group * pair_rows
    panel_rows = panel.shape[2]
    total_out = green.shape[2]
    qpoint = lax.axis_index("pb")
    freq = lax.axis_index("freq")
    x = lax.axis_index("ga")
    y, core = freq // 2, freq % 2
    ny, nx, nc = 1 - y, 1 - x, 1 - core

    def place(yy, cc, xx):
        return (yy * 2 + cc) * count_ga + xx

    me = place(y, core, x)
    at_x = {"freq": freq, "ga": nx}
    at_y = {"freq": ny * 2 + core, "ga": x}
    at_core = {"freq": y * 2 + nc, "ga": x}
    onward = {"freq": (y + core * (1 - 2 * y)) * 2 + core, "ga": x + (1 - core) * (1 - 2 * x)}
    passed = place(y + (1 - core) * (1 - 2 * y), core, x + core * (1 - 2 * x))
    from_x = place(y, core, nx)
    from_y = place(ny, core, x)
    across = place(ny, core, nx)
    mine = (me, from_x, from_y, across)
    theirs = (place(y, nc, x), place(y, nc, nx), place(ny, nc, x), place(ny, nc, nx))

    def own_copy(k):
        return pltpu.make_async_copy(
            dens_ref.at[0, :, :, pl.ds(k * width, width)], blocks.at[k, me], own_sem.at[k]
        )

    def panel_copy(k):
        return pltpu.make_async_copy(
            screen_ref.at[0, 0, :, :, pl.ds(k * width, width)], panel.at[k], panel_sem.at[k]
        )

    def remote(k, lane, block, target):
        return pltpu.make_async_remote_copy(
            src_ref=blocks.at[k, block],
            dst_ref=blocks.at[k, block],
            send_sem=send_sem.at[lane, k],
            recv_sem=recv_sem.at[lane, k],
            device_id=target,
            device_id_type=MESH,
        )

    for k in range(chunks):
        own_copy(k).start()
    for k in range(chunks):
        panel_copy(k).start()

    barrier = pltpu.get_barrier_semaphore()
    peers = []
    for step in range(1, group):
        spot = (me + step) % group
        peers.append({"freq": spot // count_ga, "ga": spot % count_ga})
    layers = []
    for step in range(1, count_pb):
        layers.append({"pb": (qpoint + step) % count_pb})
    for target in peers + layers:
        pl.semaphore_signal(barrier, inc=1, device_id=target, device_id_type=MESH)
    pl.semaphore_wait(barrier, len(peers) + len(layers))

    def send_own(k):
        own_copy(k).wait()
        remote(k, 0, me, at_x).start()
        remote(k, 1, me, at_y).start()
        remote(k, 3, me, at_core).start()

    def pass_on(k):
        remote(k, 0, from_x, at_x).wait_recv()
        remote(k, 1, from_y, at_y).wait_recv()
        remote(k, 2, passed, onward).start()
        remote(k, 4, from_x, at_core).start()
        remote(k, 5, from_y, at_core).start()

    def share_across(k):
        remote(k, 2, across, onward).wait_recv()
        remote(k, 6, across, at_core).start()

    def arrive(k):
        for which in range(4):
            remote(k, 3 + which, theirs[which], at_core).wait_recv()
        panel_copy(k).wait()

    for k in range(AHEAD):
        send_own(k)

    kpoint = kmq_ref[qpoint]
    level_row = energy_ref[pl.ds(kpoint, 1), :]
    levels = jnp.broadcast_to(level_row, (8, level_row.shape[1])).T[:, :1]
    bands = lax.broadcasted_iota(jnp.int32, (level_row.shape[1], total_out), 0)
    grid = lax.broadcasted_iota(jnp.int32, (level_row.shape[1], total_out), 1)
    omegas = -2.0 + 4.0 * grid.astype(jnp.float32) / total_out
    freq_shift = 4.0 * offset_ref[freq].astype(jnp.float32) / total_out
    real_part = omegas - freq_shift - levels
    imag_part = jnp.where(bands < filled_ref[kpoint], -broadening, broadening)
    scale = weight_ref[freq] / (2.0 * math.pi * count_pb)
    inverse = scale / (real_part * real_part + imag_part * imag_part)
    green[0] = real_part * inverse
    green[1] = -imag_part * inverse

    tiles = panel_rows // tile
    pass_on(0)
    for k in range(chunks):
        if k + AHEAD < chunks:
            send_own(k + AHEAD)
        if k + 1 < chunks:
            pass_on(k + 1)
        share_across(k)
        arrive(k)
        for plane in range(2):

            @pl.loop(0, tiles)
            def _(t):
                rows = pl.ds(pl.multiple_of(t * tile, tile), tile)
                left = blocks[k].reshape(2 * pairs, width)
                value = lax.dot_general(
                    left,
                    panel[k, plane, rows, :],
                    (((1,), (1,)), ((), ())),
                    preferred_element_type=jnp.float32,
                )
                if k == 0:
                    acc[plane, :, rows] = value
                else:
                    acc[plane, :, rows] += value

    chunks_here = panel_rows // width
    spread = 128
    sums = []
    for b in range(group):
        def add_chunk(t, totals):
            real_total, imag_total = totals
            for part in range(width // spread):
                dense = blocks[x * chunks_here + t, b, :, :, part * spread : (part + 1) * spread]
                dense = dense.astype(jnp.float32)
                cols = pl.ds(pl.multiple_of(t * width, width) + part * spread, spread)
                low = pl.ds(2 * b * pair_rows, pair_rows)
                high = pl.ds((2 * b + 1) * pair_rows, pair_rows)
                real_x = acc[0, low, cols] - acc[1, high, cols]
                imag_x = acc[1, low, cols] + acc[0, high, cols]
                real_total = real_total + dense[0] * real_x + dense[1] * imag_x
                imag_total = imag_total + dense[0] * imag_x - dense[1] * real_x
            return real_total, imag_total

        zero = jnp.zeros((pair_rows, spread), jnp.float32)
        sums.append(lax.fori_loop(0, chunks_here, add_chunk, (zero, zero)))
    pair_real = jnp.sum(jnp.concatenate([s[0] for s in sums]), axis=1, keepdims=True)
    pair_imag = jnp.sum(jnp.concatenate([s[1] for s in sums]), axis=1, keepdims=True)
    real_out = jnp.sum(pair_real * green[0] - pair_imag * green[1], axis=0, keepdims=True)
    imag_out = jnp.sum(pair_real * green[1] + pair_imag * green[0], axis=0, keepdims=True)

    plane_parts[0, 0:1] = -imag_out
    plane_parts[0, 1:2] = real_out
    copies = []
    for step in range(1, group):
        copy = pltpu.make_async_remote_copy(
            src_ref=plane_parts.at[0],
            dst_ref=plane_parts.at[step],
            send_sem=plane_send.at[step],
            recv_sem=plane_recv.at[step],
            device_id=peers[step - 1],
            device_id_type=MESH,
        )
        copy.start()
        copies.append(copy)
    for copy in copies:
        copy.wait_recv()
    pb_parts[0] = jnp.sum(plane_parts[...], axis=0)
    for step in range(1, count_pb):
        copy = pltpu.make_async_remote_copy(
            src_ref=pb_parts.at[0],
            dst_ref=pb_parts.at[step],
            send_sem=pb_send.at[step],
            recv_sem=pb_recv.at[step],
            device_id=layers[step - 1],
            device_id_type=MESH,
        )
        copy.start()
        copies.append(copy)
    for copy in copies[group - 1 :]:
        copy.wait_recv()
    total = jnp.sum(pb_parts[...], axis=0)
    first = (qpoint * count_freq + freq) * OUT_DEV
    lanes = lax.broadcasted_iota(jnp.int32, total.shape, 1)
    spots = lax.broadcasted_iota(jnp.int32, (2, OUT_DEV), 1)
    result = jnp.zeros((2, OUT_DEV), jnp.float32)
    for j in range(OUT_DEV):
        picked = jnp.sum(jnp.where(lanes == first + j, total, 0.0), axis=1, keepdims=True)
        result = jnp.where(spots == j, picked, result)
    out_ref[...] = result.reshape(out_ref.shape)

    for copy in copies:
        copy.wait_send()
    for k in range(chunks):
        remote(k, 0, me, at_x).wait_send()
        remote(k, 1, me, at_y).wait_send()
        remote(k, 2, passed, onward).wait_send()
        for which in range(4):
            remote(k, 3 + which, mine[which], at_core).wait_send()


def fused_body(densities, screened, energies, occupied, kmq, offsets, weights):
    count_pb = lax.axis_size("pb")
    count_freq = lax.axis_size("freq")
    count_ga = lax.axis_size("ga")
    pair_rows, basis = densities.shape[2:]
    panel_rows = screened.shape[3]
    group = count_freq * count_ga
    pairs = group * pair_rows
    width = basis // CHUNKS
    total_out = OUT_DEV * count_pb * count_freq
    shape = (count_pb, count_freq, count_ga, CHUNKS, width, min(TILE, panel_rows))
    anywhere = pl.BlockSpec(memory_space=pl.ANY)
    scalar = pl.BlockSpec(memory_space=pltpu.SMEM)
    vector = pl.BlockSpec(memory_space=pltpu.VMEM)
    return pl.pallas_call(
        functools.partial(fused_kernel, shape),
        out_shape=jax.ShapeDtypeStruct((2, NS, OUT_DEV), jnp.float32),
        in_specs=[anywhere, anywhere, vector, scalar, scalar, scalar, scalar],
        out_specs=vector,
        scratch_shapes=[
            pltpu.VMEM((CHUNKS, group, 2, pair_rows, width), jnp.bfloat16),
            pltpu.VMEM((CHUNKS, 2, panel_rows, width), jnp.bfloat16),
            pltpu.VMEM((2, 2 * pairs, panel_rows), jnp.float32),
            pltpu.VMEM((2, NB, total_out), jnp.float32),
            pltpu.VMEM((group, 2, total_out), jnp.float32),
            pltpu.VMEM((count_pb, 2, total_out), jnp.float32),
            pltpu.SemaphoreType.DMA((CHUNKS,)),
            pltpu.SemaphoreType.DMA((CHUNKS,)),
            pltpu.SemaphoreType.DMA((7, CHUNKS)),
            pltpu.SemaphoreType.DMA((7, CHUNKS)),
            pltpu.SemaphoreType.DMA((group,)),
            pltpu.SemaphoreType.DMA((group,)),
            pltpu.SemaphoreType.DMA((count_pb,)),
            pltpu.SemaphoreType.DMA((count_pb,)),
        ],
        compiler_params=pltpu.CompilerParams(
            collective_id=0, has_side_effects=True, vmem_limit_bytes=58 * 2**20
        ),
    )(densities, screened, energies, occupied, kmq, offsets, weights)


def body(densities, screened, *rest):
    chips = lax.axis_size("freq") == 4 and lax.axis_size("ga") == 2
    if chips and densities.shape[2] % 16 == 0 and densities.shape[3] % (CHUNKS * 128) == 0:
        return fused_body(densities, screened, *rest)
    return plain_body(densities, screened, *rest)


def solution(mesh):
    placed = (
        P("pb", None, ("freq", "ga"), None),
        P("pb", "freq", None, "ga", None),
        P(),
        P(),
        P(),
        P(),
        P(),
    )
    return jax.shard_map(
        body, mesh=mesh, in_specs=placed, out_specs=P(None, None, ("pb", "freq")), check_vma=False
    )
```

```python
import functools
import math

import jax
import jax.numpy as jnp
from jax import lax
from jax.experimental import pallas as pl
from jax.experimental.pallas import tpu as pltpu
from jax.sharding import PartitionSpec as P

MESH = pl.DeviceIdType.MESH
CHUNKS = 8
TILE = 2048
AHEAD = 3

NB = 256
NS = 1
OUT_DEV = 4


broadening = 0.15


def from_behind(block, axis, distance):
    devices = range(lax.axis_size(axis))
    route = [((i - distance) % len(devices), i) for i in devices]
    return lax.ppermute(block, axis, route)


def green_parts(level_row, filled, freq_shift, omegas):
    bands = jnp.arange(level_row.shape[0], dtype=jnp.int32)
    pole_sign = jnp.where(bands < filled, -1.0, 1.0).astype(jnp.float32)
    real_part = omegas[None, :] - freq_shift - level_row[:, None]
    imag_part = broadening * pole_sign[:, None]
    denominator = real_part * real_part + imag_part * imag_part
    return (real_part / denominator, -imag_part / denominator)


def spectrum(pair_real, pair_imag, green_real, green_imag):
    exact = lax.Precision.HIGHEST
    real_out = jnp.dot(pair_real, green_real, precision=exact) - jnp.dot(
        pair_imag, green_imag, precision=exact
    )
    imag_out = jnp.dot(pair_real, green_imag, precision=exact) + jnp.dot(
        pair_imag, green_real, precision=exact
    )
    return jnp.stack([real_out, imag_out])


def panel_product(density_all, screen):
    pair_rows = density_all.shape[1]
    panel_rows = screen.shape[1]
    product = lax.dot_general(
        density_all.reshape(2 * pair_rows, -1),
        screen.reshape(2 * panel_rows, -1),
        (((1,), (1,)), ((), ())),
        preferred_element_type=jnp.float32,
    )
    product = product.reshape(2, pair_rows, 2, panel_rows)
    return (product[0, :, 0] - product[1, :, 1], product[0, :, 1] + product[1, :, 0])


def plain_body(densities, screened, energies, occupied, kmq, offsets, weights):
    qpoint = lax.axis_index("pb")
    my_freq = lax.axis_index("freq")
    my_panel = lax.axis_index("ga")
    count_pb = lax.axis_size("pb")
    count_freq = lax.axis_size("freq")
    screen = screened[0, 0]
    panel_width = screen.shape[1]
    local_block = densities[0]
    whole = lax.all_gather(local_block, ("freq", "ga"), axis=1, tiled=True)
    real_x, imag_x = panel_product(whole, screen)
    own_rows = lax.dynamic_slice_in_dim(whole, my_panel * panel_width, panel_width, 2)
    dense = own_rows.astype(jnp.float32)
    real_sum = jnp.sum(dense[0] * real_x + dense[1] * imag_x, axis=1)
    imag_sum = jnp.sum(dense[0] * imag_x - dense[1] * real_x, axis=1)
    pair_total = lax.psum(jnp.stack([real_sum, imag_sum]), "ga")
    weighted = (pair_total * weights[my_freq]).reshape(2, NS, NB)
    kpoint = kmq[qpoint]
    level_row = energies[kpoint]
    filled = occupied[kpoint]
    total_out = OUT_DEV * count_pb * count_freq
    index_grid = (jnp.arange(count_pb, dtype=jnp.int32)[:, None] * count_freq + my_freq) * OUT_DEV
    index_grid = (index_grid + jnp.arange(OUT_DEV, dtype=jnp.int32)[None, :]).reshape(-1)
    omegas = -2.0 + 4.0 * index_grid.astype(jnp.float32) / total_out
    summed = jnp.zeros((2, NS, count_pb * OUT_DEV), jnp.float32)
    passed = weighted
    for rotation in range(count_freq):
        anchor = (my_freq - rotation) % count_freq
        freq_shift = 4.0 * offsets[anchor].astype(jnp.float32) / total_out
        green_real, green_imag = green_parts(level_row, filled, freq_shift, omegas)
        summed = summed + spectrum(passed[0], passed[1], green_real, green_imag)
        if rotation + 1 < count_freq:
            passed = from_behind(passed, "freq", 1)
    local_part = lax.psum_scatter(summed, "pb", scatter_dimension=2, tiled=True)
    prefactor = 1.0 / (2.0 * math.pi * count_pb)
    return jnp.stack([-prefactor * local_part[1], prefactor * local_part[0]])


def fused_kernel(
    shape,
    dens_ref,
    screen_ref,
    energy_ref,
    filled_ref,
    kmq_ref,
    offset_ref,
    weight_ref,
    out_ref,
    blocks,
    panel,
    acc,
    green,
    plane_parts,
    pb_parts,
    own_sem,
    panel_sem,
    send_sem,
    recv_sem,
    plane_send,
    plane_recv,
    pb_send,
    pb_recv,
):
    count_pb, count_freq, count_ga, chunks, width, tile = shape
    group = count_freq * count_ga
    pair_rows = blocks.shape[3]
    pairs = group * pair_rows
    panel_rows = panel.shape[2]
    total_out = green.shape[2]
    qpoint = lax.axis_index("pb")
    freq = lax.axis_index("freq")
    x = lax.axis_index("ga")
    y, core = freq // 2, freq % 2
    ny, nx, nc = 1 - y, 1 - x, 1 - core

    def place(yy, cc, xx):
        return (yy * 2 + cc) * count_ga + xx

    me = place(y, core, x)
    at_x = {"freq": freq, "ga": nx}
    at_y = {"freq": ny * 2 + core, "ga": x}
    at_core = {"freq": y * 2 + nc, "ga": x}
    onward = {"freq": (y + core * (1 - 2 * y)) * 2 + core, "ga": x + (1 - core) * (1 - 2 * x)}
    passed = place(y + (1 - core) * (1 - 2 * y), core, x + core * (1 - 2 * x))
    from_x = place(y, core, nx)
    from_y = place(ny, core, x)
    across = place(ny, core, nx)
    mine = (me, from_x, from_y, across)
    theirs = (place(y, nc, x), place(y, nc, nx), place(ny, nc, x), place(ny, nc, nx))

    def own_copy(k):
        return pltpu.make_async_copy(
            dens_ref.at[0, :, :, pl.ds(k * width, width)], blocks.at[k, me], own_sem.at[k]
        )

    def panel_copy(k):
        return pltpu.make_async_copy(
            screen_ref.at[0, 0, :, :, pl.ds(k * width, width)], panel.at[k], panel_sem.at[k]
        )

    def remote(k, lane, block, target):
        return pltpu.make_async_remote_copy(
            src_ref=blocks.at[k, block],
            dst_ref=blocks.at[k, block],
            send_sem=send_sem.at[lane, k],
            recv_sem=recv_sem.at[lane, k],
            device_id=target,
            device_id_type=MESH,
        )

    for k in range(chunks):
        own_copy(k).start()
    for k in range(chunks):
        panel_copy(k).start()

    barrier = pltpu.get_barrier_semaphore()
    peers = []
    for step in range(1, group):
        spot = (me + step) % group
        peers.append({"freq": spot // count_ga, "ga": spot % count_ga})
    layers = []
    for step in range(1, count_pb):
        layers.append({"pb": (qpoint + step) % count_pb})
    for target in peers + layers:
        pl.semaphore_signal(barrier, inc=1, device_id=target, device_id_type=MESH)
    pl.semaphore_wait(barrier, len(peers) + len(layers))

    def send_own(k):
        own_copy(k).wait()
        remote(k, 0, me, at_x).start()
        remote(k, 1, me, at_y).start()
        remote(k, 3, me, at_core).start()

    def pass_on(k):
        remote(k, 0, from_x, at_x).wait_recv()
        remote(k, 1, from_y, at_y).wait_recv()
        remote(k, 2, passed, onward).start()
        remote(k, 4, from_x, at_core).start()
        remote(k, 5, from_y, at_core).start()

    def share_across(k):
        remote(k, 2, across, onward).wait_recv()
        remote(k, 6, across, at_core).start()

    def arrive(k):
        for which in range(4):
            remote(k, 3 + which, theirs[which], at_core).wait_recv()
        panel_copy(k).wait()

    for k in range(AHEAD):
        send_own(k)

    kpoint = kmq_ref[qpoint]
    level_row = energy_ref[pl.ds(kpoint, 1), :]
    levels = jnp.broadcast_to(level_row, (8, level_row.shape[1])).T[:, :1]
    bands = lax.broadcasted_iota(jnp.int32, (level_row.shape[1], total_out), 0)
    grid = lax.broadcasted_iota(jnp.int32, (level_row.shape[1], total_out), 1)
    omegas = -2.0 + 4.0 * grid.astype(jnp.float32) / total_out
    freq_shift = 4.0 * offset_ref[freq].astype(jnp.float32) / total_out
    real_part = omegas - freq_shift - levels
    imag_part = jnp.where(bands < filled_ref[kpoint], -broadening, broadening)
    scale = weight_ref[freq] / (2.0 * math.pi * count_pb)
    inverse = scale / (real_part * real_part + imag_part * imag_part)
    green[0] = real_part * inverse
    green[1] = -imag_part * inverse

    tiles = panel_rows // tile
    pass_on(0)
    for k in range(chunks):
        if k + AHEAD < chunks:
            send_own(k + AHEAD)
        if k + 1 < chunks:
            pass_on(k + 1)
        share_across(k)
        arrive(k)
        for plane in range(2):

            @pl.loop(0, tiles)
            def _(t):
                rows = pl.ds(pl.multiple_of(t * tile, tile), tile)
                left = blocks[k].reshape(2 * pairs, width)
                value = lax.dot_general(
                    left,
                    panel[k, plane, rows, :],
                    (((1,), (1,)), ((), ())),
                    preferred_element_type=jnp.float32,
                )
                if k == 0:
                    acc[plane, :, rows] = value
                else:
                    acc[plane, :, rows] += value

    chunks_here = panel_rows // width
    spread = 128
    sums = []
    for b in range(group):
        def add_chunk(t, totals):
            real_total, imag_total = totals
            for part in range(width // spread):
                dense = blocks[x * chunks_here + t, b, :, :, part * spread : (part + 1) * spread]
                dense = dense.astype(jnp.float32)
                cols = pl.ds(pl.multiple_of(t * width, width) + part * spread, spread)
                low = pl.ds(2 * b * pair_rows, pair_rows)
                high = pl.ds((2 * b + 1) * pair_rows, pair_rows)
                real_x = acc[0, low, cols] - acc[1, high, cols]
                imag_x = acc[1, low, cols] + acc[0, high, cols]
                real_total = real_total + dense[0] * real_x + dense[1] * imag_x
                imag_total = imag_total + dense[0] * imag_x - dense[1] * real_x
            return real_total, imag_total

        zero = jnp.zeros((pair_rows, spread), jnp.float32)
        sums.append(lax.fori_loop(0, chunks_here, add_chunk, (zero, zero)))
    pair_real = jnp.sum(jnp.concatenate([s[0] for s in sums]), axis=1, keepdims=True)
    pair_imag = jnp.sum(jnp.concatenate([s[1] for s in sums]), axis=1, keepdims=True)
    real_out = jnp.sum(pair_real * green[0] - pair_imag * green[1], axis=0, keepdims=True)
    imag_out = jnp.sum(pair_real * green[1] + pair_imag * green[0], axis=0, keepdims=True)

    plane_parts[0, 0:1] = -imag_out
    plane_parts[0, 1:2] = real_out
    copies = []
    for step in range(1, group):
        copy = pltpu.make_async_remote_copy(
            src_ref=plane_parts.at[0],
            dst_ref=plane_parts.at[step],
            send_sem=plane_send.at[step],
            recv_sem=plane_recv.at[step],
            device_id=peers[step - 1],
            device_id_type=MESH,
        )
        copy.start()
        copies.append(copy)
    for copy in copies:
        copy.wait_recv()
    pb_parts[0] = jnp.sum(plane_parts[...], axis=0)
    for step in range(1, count_pb):
        copy = pltpu.make_async_remote_copy(
            src_ref=pb_parts.at[0],
            dst_ref=pb_parts.at[step],
            send_sem=pb_send.at[step],
            recv_sem=pb_recv.at[step],
            device_id=layers[step - 1],
            device_id_type=MESH,
        )
        copy.start()
        copies.append(copy)
    for copy in copies[group - 1 :]:
        copy.wait_recv()
    total = jnp.sum(pb_parts[...], axis=0)
    first = (qpoint * count_freq + freq) * OUT_DEV
    lanes = lax.broadcasted_iota(jnp.int32, total.shape, 1)
    spots = lax.broadcasted_iota(jnp.int32, (2, OUT_DEV), 1)
    result = jnp.zeros((2, OUT_DEV), jnp.float32)
    for j in range(OUT_DEV):
        picked = jnp.sum(jnp.where(lanes == first + j, total, 0.0), axis=1, keepdims=True)
        result = jnp.where(spots == j, picked, result)
    out_ref[...] = result.reshape(out_ref.shape)

    for copy in copies:
        copy.wait_send()
    for k in range(chunks):
        remote(k, 0, me, at_x).wait_send()
        remote(k, 1, me, at_y).wait_send()
        remote(k, 2, passed, onward).wait_send()
        for which in range(4):
            remote(k, 3 + which, mine[which], at_core).wait_send()


def fused_body(densities, screened, energies, occupied, kmq, offsets, weights):
    count_pb = lax.axis_size("pb")
    count_freq = lax.axis_size("freq")
    count_ga = lax.axis_size("ga")
    pair_rows, basis = densities.shape[2:]
    panel_rows = screened.shape[3]
    group = count_freq * count_ga
    pairs = group * pair_rows
    width = basis // CHUNKS
    total_out = OUT_DEV * count_pb * count_freq
    shape = (count_pb, count_freq, count_ga, CHUNKS, width, min(TILE, panel_rows))
    anywhere = pl.BlockSpec(memory_space=pl.ANY)
    scalar = pl.BlockSpec(memory_space=pltpu.SMEM)
    vector = pl.BlockSpec(memory_space=pltpu.VMEM)
    return pl.pallas_call(
        functools.partial(fused_kernel, shape),
        out_shape=jax.ShapeDtypeStruct((2, NS, OUT_DEV), jnp.float32),
        in_specs=[anywhere, anywhere, vector, scalar, scalar, scalar, scalar],
        out_specs=vector,
        scratch_shapes=[
            pltpu.VMEM((CHUNKS, group, 2, pair_rows, width), jnp.bfloat16),
            pltpu.VMEM((CHUNKS, 2, panel_rows, width), jnp.bfloat16),
            pltpu.VMEM((2, 2 * pairs, panel_rows), jnp.float32),
            pltpu.VMEM((2, NB, total_out), jnp.float32),
            pltpu.VMEM((group, 2, total_out), jnp.float32),
            pltpu.VMEM((count_pb, 2, total_out), jnp.float32),
            pltpu.SemaphoreType.DMA((CHUNKS,)),
            pltpu.SemaphoreType.DMA((CHUNKS,)),
            pltpu.SemaphoreType.DMA((7, CHUNKS)),
            pltpu.SemaphoreType.DMA((7, CHUNKS)),
            pltpu.SemaphoreType.DMA((group,)),
            pltpu.SemaphoreType.DMA((group,)),
            pltpu.SemaphoreType.DMA((count_pb,)),
            pltpu.SemaphoreType.DMA((count_pb,)),
        ],
        compiler_params=pltpu.CompilerParams(
            collective_id=0, has_side_effects=True, vmem_limit_bytes=58 * 2**20
        ),
    )(densities, screened, energies, occupied, kmq, offsets, weights)


def body(densities, screened, *rest):
    chips = lax.axis_size("freq") == 4 and lax.axis_size("ga") == 2
    if chips and densities.shape[2] % 16 == 0 and densities.shape[3] % (CHUNKS * 128) == 0:
        return fused_body(densities, screened, *rest)
    return plain_body(densities, screened, *rest)


def solution(mesh):
    placed = (
        P("pb", None, ("freq", "ga"), None),
        P("pb", "freq", None, "ga", None),
        P(),
        P(),
        P(),
        P(),
        P(),
    )
    return jax.shard_map(
        body, mesh=mesh, in_specs=placed, out_specs=P(None, None, ("pb", "freq")), check_vma=False
    )
```

```python
import functools
import math

import jax
import jax.numpy as jnp
from jax import lax
from jax.experimental import pallas as pl
from jax.experimental.pallas import tpu as pltpu
from jax.sharding import PartitionSpec as P

MESH = pl.DeviceIdType.MESH
CHUNKS = 8
TILE = 2048
AHEAD = 3

NB = 256
NS = 1
OUT_DEV = 4


broadening = 0.15


def from_behind(block, axis, distance):
    devices = range(lax.axis_size(axis))
    route = [((i - distance) % len(devices), i) for i in devices]
    return lax.ppermute(block, axis, route)


def green_parts(level_row, filled, freq_shift, omegas):
    bands = jnp.arange(level_row.shape[0], dtype=jnp.int32)
    pole_sign = jnp.where(bands < filled, -1.0, 1.0).astype(jnp.float32)
    real_part = omegas[None, :] - freq_shift - level_row[:, None]
    imag_part = broadening * pole_sign[:, None]
    denominator = real_part * real_part + imag_part * imag_part
    return (real_part / denominator, -imag_part / denominator)


def spectrum(pair_real, pair_imag, green_real, green_imag):
    exact = lax.Precision.HIGHEST
    real_out = jnp.dot(pair_real, green_real, precision=exact) - jnp.dot(
        pair_imag, green_imag, precision=exact
    )
    imag_out = jnp.dot(pair_real, green_imag, precision=exact) + jnp.dot(
        pair_imag, green_real, precision=exact
    )
    return jnp.stack([real_out, imag_out])


def panel_product(density_all, screen):
    pair_rows = density_all.shape[1]
    panel_rows = screen.shape[1]
    product = lax.dot_general(
        density_all.reshape(2 * pair_rows, -1),
        screen.reshape(2 * panel_rows, -1),
        (((1,), (1,)), ((), ())),
        preferred_element_type=jnp.float32,
    )
    product = product.reshape(2, pair_rows, 2, panel_rows)
    return (product[0, :, 0] - product[1, :, 1], product[0, :, 1] + product[1, :, 0])


def plain_body(densities, screened, energies, occupied, kmq, offsets, weights):
    qpoint = lax.axis_index("pb")
    my_freq = lax.axis_index("freq")
    my_panel = lax.axis_index("ga")
    count_pb = lax.axis_size("pb")
    count_freq = lax.axis_size("freq")
    screen = screened[0, 0]
    panel_width = screen.shape[1]
    local_block = densities[0]
    whole = lax.all_gather(local_block, ("freq", "ga"), axis=1, tiled=True)
    real_x, imag_x = panel_product(whole, screen)
    own_rows = lax.dynamic_slice_in_dim(whole, my_panel * panel_width, panel_width, 2)
    dense = own_rows.astype(jnp.float32)
    real_sum = jnp.sum(dense[0] * real_x + dense[1] * imag_x, axis=1)
    imag_sum = jnp.sum(dense[0] * imag_x - dense[1] * real_x, axis=1)
    pair_total = lax.psum(jnp.stack([real_sum, imag_sum]), "ga")
    weighted = (pair_total * weights[my_freq]).reshape(2, NS, NB)
    kpoint = kmq[qpoint]
    level_row = energies[kpoint]
    filled = occupied[kpoint]
    total_out = OUT_DEV * count_pb * count_freq
    index_grid = (jnp.arange(count_pb, dtype=jnp.int32)[:, None] * count_freq + my_freq) * OUT_DEV
    index_grid = (index_grid + jnp.arange(OUT_DEV, dtype=jnp.int32)[None, :]).reshape(-1)
    omegas = -2.0 + 4.0 * index_grid.astype(jnp.float32) / total_out
    summed = jnp.zeros((2, NS, count_pb * OUT_DEV), jnp.float32)
    passed = weighted
    for rotation in range(count_freq):
        anchor = (my_freq - rotation) % count_freq
        freq_shift = 4.0 * offsets[anchor].astype(jnp.float32) / total_out
        green_real, green_imag = green_parts(level_row, filled, freq_shift, omegas)
        summed = summed + spectrum(passed[0], passed[1], green_real, green_imag)
        if rotation + 1 < count_freq:
            passed = from_behind(passed, "freq", 1)
    local_part = lax.psum_scatter(summed, "pb", scatter_dimension=2, tiled=True)
    prefactor = 1.0 / (2.0 * math.pi * count_pb)
    return jnp.stack([-prefactor * local_part[1], prefactor * local_part[0]])


def fused_kernel(
    shape,
    dens_ref,
    screen_ref,
    energy_ref,
    filled_ref,
    kmq_ref,
    offset_ref,
    weight_ref,
    out_ref,
    blocks,
    panel,
    acc,
    green,
    parts,
    own_sem,
    panel_sem,
    send_sem,
    recv_sem,
    part_send,
    part_recv,
):
    count_pb, count_freq, count_ga, chunks, width, tile = shape
    group = count_freq * count_ga
    pair_rows = blocks.shape[3]
    pairs = group * pair_rows
    panel_rows = panel.shape[2]
    total_out = green.shape[2]
    qpoint = lax.axis_index("pb")
    freq = lax.axis_index("freq")
    x = lax.axis_index("ga")
    y, core = freq // 2, freq % 2
    ny, nx, nc = 1 - y, 1 - x, 1 - core

    def place(yy, cc, xx):
        return (yy * 2 + cc) * count_ga + xx

    me = place(y, core, x)
    at_x = {"freq": freq, "ga": nx}
    at_y = {"freq": ny * 2 + core, "ga": x}
    at_core = {"freq": y * 2 + nc, "ga": x}
    onward = {"freq": (y + core * (1 - 2 * y)) * 2 + core, "ga": x + (1 - core) * (1 - 2 * x)}
    passed = place(y + (1 - core) * (1 - 2 * y), core, x + core * (1 - 2 * x))
    from_x = place(y, core, nx)
    from_y = place(ny, core, x)
    across = place(ny, core, nx)
    mine = (me, from_x, from_y, across)
    theirs = (place(y, nc, x), place(y, nc, nx), place(ny, nc, x), place(ny, nc, nx))

    def own_copy(k):
        return pltpu.make_async_copy(
            dens_ref.at[0, :, :, pl.ds(k * width, width)], blocks.at[k, me], own_sem.at[k]
        )

    def panel_copy(k):
        return pltpu.make_async_copy(
            screen_ref.at[0, 0, :, :, pl.ds(k * width, width)], panel.at[k], panel_sem.at[k]
        )

    def remote(k, lane, block, target):
        return pltpu.make_async_remote_copy(
            src_ref=blocks.at[k, block],
            dst_ref=blocks.at[k, block],
            send_sem=send_sem.at[lane, k],
            recv_sem=recv_sem.at[lane, k],
            device_id=target,
            device_id_type=MESH,
        )

    for k in range(chunks):
        own_copy(k).start()
    for k in range(chunks):
        panel_copy(k).start()

    barrier = pltpu.get_barrier_semaphore()
    peers = []
    for step in range(1, count_pb * group):
        layer = (qpoint + step // group) % count_pb
        spot = (me + step) % group
        peers.append({"pb": layer, "freq": spot // count_ga, "ga": spot % count_ga})
    for target in peers:
        pl.semaphore_signal(barrier, inc=1, device_id=target, device_id_type=MESH)
    pl.semaphore_wait(barrier, len(peers))

    def send_own(k):
        own_copy(k).wait()
        remote(k, 0, me, at_x).start()
        remote(k, 1, me, at_y).start()
        remote(k, 3, me, at_core).start()

    def pass_on(k):
        remote(k, 0, from_x, at_x).wait_recv()
        remote(k, 1, from_y, at_y).wait_recv()
        remote(k, 2, passed, onward).start()
        remote(k, 4, from_x, at_core).start()
        remote(k, 5, from_y, at_core).start()

    def share_across(k):
        remote(k, 2, across, onward).wait_recv()
        remote(k, 6, across, at_core).start()

    def arrive(k):
        for which in range(4):
            remote(k, 3 + which, theirs[which], at_core).wait_recv()
        panel_copy(k).wait()

    for k in range(AHEAD):
        send_own(k)

    kpoint = kmq_ref[qpoint]
    level_row = energy_ref[pl.ds(kpoint, 1), :]
    levels = jnp.broadcast_to(level_row, (8, level_row.shape[1])).T[:, :1]
    bands = lax.broadcasted_iota(jnp.int32, (level_row.shape[1], total_out), 0)
    grid = lax.broadcasted_iota(jnp.int32, (level_row.shape[1], total_out), 1)
    omegas = -2.0 + 4.0 * grid.astype(jnp.float32) / total_out
    freq_shift = 4.0 * offset_ref[freq].astype(jnp.float32) / total_out
    real_part = omegas - freq_shift - levels
    imag_part = jnp.where(bands < filled_ref[kpoint], -broadening, broadening)
    scale = weight_ref[freq] / (2.0 * math.pi * count_pb)
    inverse = scale / (real_part * real_part + imag_part * imag_part)
    green[0] = real_part * inverse
    green[1] = -imag_part * inverse

    tiles = panel_rows // tile
    pass_on(0)
    pass_on(1)
    share_across(0)
    for k in range(chunks):
        if k + AHEAD < chunks:
            send_own(k + AHEAD)
        arrive(k)
        for plane in range(2):
            if plane == 1:
                if k + 2 < chunks:
                    pass_on(k + 2)
                if k + 1 < chunks:
                    share_across(k + 1)

            @pl.loop(0, tiles)
            def _(t):
                rows = pl.ds(pl.multiple_of(t * tile, tile), tile)
                left = blocks[k].reshape(2 * pairs, width)
                value = lax.dot_general(
                    left,
                    panel[k, plane, rows, :],
                    (((1,), (1,)), ((), ())),
                    preferred_element_type=jnp.float32,
                )
                if k == 0:
                    acc[plane, :, rows] = value
                else:
                    acc[plane, :, rows] += value

    chunks_here = panel_rows // width
    spread = 128
    sums = []
    for b in range(group):
        def add_chunk(t, totals):
            real_total, imag_total = totals
            for part in range(width // spread):
                dense = blocks[x * chunks_here + t, b, :, :, part * spread : (part + 1) * spread]
                dense = dense.astype(jnp.float32)
                cols = pl.ds(pl.multiple_of(t * width, width) + part * spread, spread)
                low = pl.ds(2 * b * pair_rows, pair_rows)
                high = pl.ds((2 * b + 1) * pair_rows, pair_rows)
                real_x = acc[0, low, cols] - acc[1, high, cols]
                imag_x = acc[1, low, cols] + acc[0, high, cols]
                real_total = real_total + dense[0] * real_x + dense[1] * imag_x
                imag_total = imag_total + dense[0] * imag_x - dense[1] * real_x
            return real_total, imag_total

        zero = jnp.zeros((pair_rows, spread), jnp.float32)
        sums.append(lax.fori_loop(0, chunks_here, add_chunk, (zero, zero)))
    pair_real = jnp.sum(jnp.concatenate([s[0] for s in sums]), axis=1, keepdims=True)
    pair_imag = jnp.sum(jnp.concatenate([s[1] for s in sums]), axis=1, keepdims=True)
    real_out = jnp.sum(pair_real * green[0] - pair_imag * green[1], axis=0, keepdims=True)
    imag_out = jnp.sum(pair_real * green[1] + pair_imag * green[0], axis=0, keepdims=True)

    parts[0, 0:1] = -imag_out
    parts[0, 1:2] = real_out
    copies = []
    for step, target in enumerate(peers, 1):
        copy = pltpu.make_async_remote_copy(
            src_ref=parts.at[0],
            dst_ref=parts.at[step],
            send_sem=part_send.at[step],
            recv_sem=part_recv.at[step],
            device_id=target,
            device_id_type=MESH,
        )
        copy.start()
        copies.append(copy)
    for copy in copies:
        copy.wait_recv()
    total = jnp.sum(parts[...], axis=0)
    first = (qpoint * count_freq + freq) * OUT_DEV
    lanes = lax.broadcasted_iota(jnp.int32, total.shape, 1)
    spots = lax.broadcasted_iota(jnp.int32, (2, OUT_DEV), 1)
    result = jnp.zeros((2, OUT_DEV), jnp.float32)
    for j in range(OUT_DEV):
        picked = jnp.sum(jnp.where(lanes == first + j, total, 0.0), axis=1, keepdims=True)
        result = jnp.where(spots == j, picked, result)
    out_ref[...] = result.reshape(out_ref.shape)

    for copy in copies:
        copy.wait_send()
    for k in range(chunks):
        remote(k, 0, me, at_x).wait_send()
        remote(k, 1, me, at_y).wait_send()
        remote(k, 2, passed, onward).wait_send()
        for which in range(4):
            remote(k, 3 + which, mine[which], at_core).wait_send()


def fused_body(densities, screened, energies, occupied, kmq, offsets, weights):
    count_pb = lax.axis_size("pb")
    count_freq = lax.axis_size("freq")
    count_ga = lax.axis_size("ga")
    pair_rows, basis = densities.shape[2:]
    panel_rows = screened.shape[3]
    group = count_freq * count_ga
    pairs = group * pair_rows
    width = basis // CHUNKS
    total_out = OUT_DEV * count_pb * count_freq
    shape = (count_pb, count_freq, count_ga, CHUNKS, width, min(TILE, panel_rows))
    anywhere = pl.BlockSpec(memory_space=pl.ANY)
    scalar = pl.BlockSpec(memory_space=pltpu.SMEM)
    vector = pl.BlockSpec(memory_space=pltpu.VMEM)
    return pl.pallas_call(
        functools.partial(fused_kernel, shape),
        out_shape=jax.ShapeDtypeStruct((2, NS, OUT_DEV), jnp.float32),
        in_specs=[anywhere, anywhere, vector, scalar, scalar, scalar, scalar],
        out_specs=vector,
        scratch_shapes=[
            pltpu.VMEM((CHUNKS, group, 2, pair_rows, width), jnp.bfloat16),
            pltpu.VMEM((CHUNKS, 2, panel_rows, width), jnp.bfloat16),
            pltpu.VMEM((2, 2 * pairs, panel_rows), jnp.float32),
            pltpu.VMEM((2, NB, total_out), jnp.float32),
            pltpu.VMEM((count_pb * group, 2, total_out), jnp.float32),
            pltpu.SemaphoreType.DMA((CHUNKS,)),
            pltpu.SemaphoreType.DMA((CHUNKS,)),
            pltpu.SemaphoreType.DMA((7, CHUNKS)),
            pltpu.SemaphoreType.DMA((7, CHUNKS)),
            pltpu.SemaphoreType.DMA((count_pb * group,)),
            pltpu.SemaphoreType.DMA((count_pb * group,)),
        ],
        compiler_params=pltpu.CompilerParams(
            collective_id=0, has_side_effects=True, vmem_limit_bytes=58 * 2**20
        ),
    )(densities, screened, energies, occupied, kmq, offsets, weights)


def body(densities, screened, *rest):
    chips = lax.axis_size("freq") == 4 and lax.axis_size("ga") == 2
    if chips and densities.shape[2] % 16 == 0 and densities.shape[3] % (CHUNKS * 128) == 0:
        return fused_body(densities, screened, *rest)
    return plain_body(densities, screened, *rest)


def solution(mesh):
    placed = (
        P("pb", None, ("freq", "ga"), None),
        P("pb", "freq", None, "ga", None),
        P(),
        P(),
        P(),
        P(),
        P(),
    )
    return jax.shard_map(
        body, mesh=mesh, in_specs=placed, out_specs=P(None, None, ("pb", "freq")), check_vma=False
    )
```

```python
import functools
import math

import jax
import jax.numpy as jnp
from jax import lax
from jax.experimental import pallas as pl
from jax.experimental.pallas import tpu as pltpu
from jax.sharding import PartitionSpec as P

MESH = pl.DeviceIdType.MESH
CHUNKS = 8
TILE = 2048
AHEAD = 4

NB = 256
NS = 1
OUT_DEV = 4


broadening = 0.15


def from_behind(block, axis, distance):
    devices = range(lax.axis_size(axis))
    route = [((i - distance) % len(devices), i) for i in devices]
    return lax.ppermute(block, axis, route)


def green_parts(level_row, filled, freq_shift, omegas):
    bands = jnp.arange(level_row.shape[0], dtype=jnp.int32)
    pole_sign = jnp.where(bands < filled, -1.0, 1.0).astype(jnp.float32)
    real_part = omegas[None, :] - freq_shift - level_row[:, None]
    imag_part = broadening * pole_sign[:, None]
    denominator = real_part * real_part + imag_part * imag_part
    return (real_part / denominator, -imag_part / denominator)


def spectrum(pair_real, pair_imag, green_real, green_imag):
    exact = lax.Precision.HIGHEST
    real_out = jnp.dot(pair_real, green_real, precision=exact) - jnp.dot(
        pair_imag, green_imag, precision=exact
    )
    imag_out = jnp.dot(pair_real, green_imag, precision=exact) + jnp.dot(
        pair_imag, green_real, precision=exact
    )
    return jnp.stack([real_out, imag_out])


def panel_product(density_all, screen):
    pair_rows = density_all.shape[1]
    panel_rows = screen.shape[1]
    product = lax.dot_general(
        density_all.reshape(2 * pair_rows, -1),
        screen.reshape(2 * panel_rows, -1),
        (((1,), (1,)), ((), ())),
        preferred_element_type=jnp.float32,
    )
    product = product.reshape(2, pair_rows, 2, panel_rows)
    return (product[0, :, 0] - product[1, :, 1], product[0, :, 1] + product[1, :, 0])


def plain_body(densities, screened, energies, occupied, kmq, offsets, weights):
    qpoint = lax.axis_index("pb")
    my_freq = lax.axis_index("freq")
    my_panel = lax.axis_index("ga")
    count_pb = lax.axis_size("pb")
    count_freq = lax.axis_size("freq")
    screen = screened[0, 0]
    panel_width = screen.shape[1]
    local_block = densities[0]
    whole = lax.all_gather(local_block, ("freq", "ga"), axis=1, tiled=True)
    real_x, imag_x = panel_product(whole, screen)
    own_rows = lax.dynamic_slice_in_dim(whole, my_panel * panel_width, panel_width, 2)
    dense = own_rows.astype(jnp.float32)
    real_sum = jnp.sum(dense[0] * real_x + dense[1] * imag_x, axis=1)
    imag_sum = jnp.sum(dense[0] * imag_x - dense[1] * real_x, axis=1)
    pair_total = lax.psum(jnp.stack([real_sum, imag_sum]), "ga")
    weighted = (pair_total * weights[my_freq]).reshape(2, NS, NB)
    kpoint = kmq[qpoint]
    level_row = energies[kpoint]
    filled = occupied[kpoint]
    total_out = OUT_DEV * count_pb * count_freq
    index_grid = (jnp.arange(count_pb, dtype=jnp.int32)[:, None] * count_freq + my_freq) * OUT_DEV
    index_grid = (index_grid + jnp.arange(OUT_DEV, dtype=jnp.int32)[None, :]).reshape(-1)
    omegas = -2.0 + 4.0 * index_grid.astype(jnp.float32) / total_out
    summed = jnp.zeros((2, NS, count_pb * OUT_DEV), jnp.float32)
    passed = weighted
    for rotation in range(count_freq):
        anchor = (my_freq - rotation) % count_freq
        freq_shift = 4.0 * offsets[anchor].astype(jnp.float32) / total_out
        green_real, green_imag = green_parts(level_row, filled, freq_shift, omegas)
        summed = summed + spectrum(passed[0], passed[1], green_real, green_imag)
        if rotation + 1 < count_freq:
            passed = from_behind(passed, "freq", 1)
    local_part = lax.psum_scatter(summed, "pb", scatter_dimension=2, tiled=True)
    prefactor = 1.0 / (2.0 * math.pi * count_pb)
    return jnp.stack([-prefactor * local_part[1], prefactor * local_part[0]])


def fused_kernel(
    shape,
    dens_ref,
    screen_ref,
    energy_ref,
    filled_ref,
    kmq_ref,
    offset_ref,
    weight_ref,
    out_ref,
    blocks,
    panel,
    acc,
    green,
    parts,
    own_sem,
    panel_sem,
    send_sem,
    recv_sem,
    part_send,
    part_recv,
    ready,
):
    count_pb, count_freq, count_ga, chunks, width, tile = shape
    group = count_freq * count_ga
    pair_rows = blocks.shape[3]
    pairs = group * pair_rows
    panel_rows = panel.shape[2]
    total_out = green.shape[2]
    qpoint = lax.axis_index("pb")
    freq = lax.axis_index("freq")
    x = lax.axis_index("ga")
    y, core = freq // 2, freq % 2
    ny, nx, nc = 1 - y, 1 - x, 1 - core

    def place(yy, cc, xx):
        return (yy * 2 + cc) * count_ga + xx

    me = place(y, core, x)
    at_x = {"freq": freq, "ga": nx}
    at_y = {"freq": ny * 2 + core, "ga": x}
    at_core = {"freq": y * 2 + nc, "ga": x}
    onward = {"freq": (y + core * (1 - 2 * y)) * 2 + core, "ga": x + (1 - core) * (1 - 2 * x)}
    passed = place(y + (1 - core) * (1 - 2 * y), core, x + core * (1 - 2 * x))
    from_x = place(y, core, nx)
    from_y = place(ny, core, x)
    across = place(ny, core, nx)
    mine = (me, from_x, from_y, across)
    theirs = (place(y, nc, x), place(y, nc, nx), place(ny, nc, x), place(ny, nc, nx))

    def own_copy(k):
        return pltpu.make_async_copy(
            dens_ref.at[0, :, :, pl.ds(k * width, width)], blocks.at[k, me], own_sem.at[k]
        )

    def panel_copy(k):
        return pltpu.make_async_copy(
            screen_ref.at[0, 0, :, :, pl.ds(k * width, width)], panel.at[k], panel_sem.at[k]
        )

    def remote(k, lane, block, target):
        return pltpu.make_async_remote_copy(
            src_ref=blocks.at[k, block],
            dst_ref=blocks.at[k, block],
            send_sem=send_sem.at[lane, k],
            recv_sem=recv_sem.at[lane, k],
            device_id=target,
            device_id_type=MESH,
        )

    for k in range(chunks):
        own_copy(k).start()
    for k in range(chunks):
        panel_copy(k).start()

    barrier = pltpu.get_barrier_semaphore()
    peers = []
    for step in range(1, count_pb * group):
        layer = (qpoint + step // group) % count_pb
        spot = (me + step) % group
        peers.append({"pb": layer, "freq": spot // count_ga, "ga": spot % count_ga})
    layers = [{"pb": (qpoint + step) % count_pb} for step in range(1, count_pb)]
    near = [at_x, at_y, at_core] + layers
    for target in near:
        pl.semaphore_signal(barrier, inc=1, device_id=target, device_id_type=MESH)
    pl.semaphore_wait(barrier, len(near))

    def send_own(k):
        own_copy(k).wait()
        remote(k, 0, me, at_x).start()
        remote(k, 1, me, at_y).start()
        remote(k, 3, me, at_core).start()

    def pass_on(k):
        remote(k, 0, from_x, at_x).wait_recv()
        remote(k, 1, from_y, at_y).wait_recv()
        remote(k, 2, passed, onward).start()
        remote(k, 4, from_x, at_core).start()
        remote(k, 5, from_y, at_core).start()

    def share_across(k):
        remote(k, 2, across, onward).wait_recv()
        remote(k, 6, across, at_core).start()

    def arrive(k):
        for which in range(4):
            remote(k, 3 + which, theirs[which], at_core).wait_recv()
        panel_copy(k).wait()

    for k in range(AHEAD):
        send_own(k)

    kpoint = kmq_ref[qpoint]
    level_row = energy_ref[pl.ds(kpoint, 1), :]
    levels = jnp.broadcast_to(level_row, (8, level_row.shape[1])).T[:, :1]
    bands = lax.broadcasted_iota(jnp.int32, (level_row.shape[1], total_out), 0)
    grid = lax.broadcasted_iota(jnp.int32, (level_row.shape[1], total_out), 1)
    omegas = -2.0 + 4.0 * grid.astype(jnp.float32) / total_out
    freq_shift = 4.0 * offset_ref[freq].astype(jnp.float32) / total_out
    real_part = omegas - freq_shift - levels
    imag_part = jnp.where(bands < filled_ref[kpoint], -broadening, broadening)
    scale = weight_ref[freq] / (2.0 * math.pi * count_pb)
    inverse = scale / (real_part * real_part + imag_part * imag_part)
    green[0] = real_part * inverse
    green[1] = -imag_part * inverse

    tiles = panel_rows // tile
    pass_on(0)
    pass_on(1)
    share_across(0)
    for k in range(chunks):
        if k + AHEAD < chunks:
            send_own(k + AHEAD)
        if k + 2 < chunks:
            pass_on(k + 2)
        arrive(k)
        if k == chunks - 2:
            for target in layers:
                pl.semaphore_signal(ready, inc=1, device_id=target, device_id_type=MESH)
        for plane in range(2):
            if plane == 1:
                if k + 1 < chunks:
                    share_across(k + 1)

            @pl.loop(0, tiles)
            def _(t):
                rows = pl.ds(pl.multiple_of(t * tile, tile), tile)
                left = blocks[k].reshape(2 * pairs, width)
                value = lax.dot_general(
                    left,
                    panel[k, plane, rows, :],
                    (((1,), (1,)), ((), ())),
                    preferred_element_type=jnp.float32,
                )
                if k == 0:
                    acc[plane, :, rows] = value
                else:
                    acc[plane, :, rows] += value

    chunks_here = panel_rows // width
    spread = 128
    sums = []
    for b in range(group):
        def add_chunk(t, totals):
            real_total, imag_total = totals
            for part in range(width // spread):
                dense = blocks[x * chunks_here + t, b, :, :, part * spread : (part + 1) * spread]
                dense = dense.astype(jnp.float32)
                cols = pl.ds(pl.multiple_of(t * width, width) + part * spread, spread)
                low = pl.ds(2 * b * pair_rows, pair_rows)
                high = pl.ds((2 * b + 1) * pair_rows, pair_rows)
                real_x = acc[0, low, cols] - acc[1, high, cols]
                imag_x = acc[1, low, cols] + acc[0, high, cols]
                real_total = real_total + dense[0] * real_x + dense[1] * imag_x
                imag_total = imag_total + dense[0] * imag_x - dense[1] * real_x
            return real_total, imag_total

        zero = jnp.zeros((pair_rows, spread), jnp.float32)
        sums.append(lax.fori_loop(0, chunks_here, add_chunk, (zero, zero)))
    pair_real = jnp.sum(jnp.concatenate([s[0] for s in sums]), axis=1, keepdims=True)
    pair_imag = jnp.sum(jnp.concatenate([s[1] for s in sums]), axis=1, keepdims=True)
    real_out = jnp.sum(pair_real * green[0] - pair_imag * green[1], axis=0, keepdims=True)
    imag_out = jnp.sum(pair_real * green[1] + pair_imag * green[0], axis=0, keepdims=True)

    parts[0, 0:1] = -imag_out
    parts[0, 1:2] = real_out
    pl.semaphore_wait(ready, len(layers))
    copies = []
    for step, target in enumerate(peers, 1):
        copy = pltpu.make_async_remote_copy(
            src_ref=parts.at[0],
            dst_ref=parts.at[step],
            send_sem=part_send.at[step],
            recv_sem=part_recv.at[step],
            device_id=target,
            device_id_type=MESH,
        )
        copy.start()
        copies.append(copy)
    for copy in copies:
        copy.wait_recv()
    total = jnp.sum(parts[...], axis=0)
    first = (qpoint * count_freq + freq) * OUT_DEV
    lanes = lax.broadcasted_iota(jnp.int32, total.shape, 1)
    spots = lax.broadcasted_iota(jnp.int32, (2, OUT_DEV), 1)
    result = jnp.zeros((2, OUT_DEV), jnp.float32)
    for j in range(OUT_DEV):
        picked = jnp.sum(jnp.where(lanes == first + j, total, 0.0), axis=1, keepdims=True)
        result = jnp.where(spots == j, picked, result)
    out_ref[...] = result.reshape(out_ref.shape)

    for copy in copies:
        copy.wait_send()
    for k in range(chunks):
        remote(k, 0, me, at_x).wait_send()
        remote(k, 1, me, at_y).wait_send()
        remote(k, 2, passed, onward).wait_send()
        for which in range(4):
            remote(k, 3 + which, mine[which], at_core).wait_send()


def fused_body(densities, screened, energies, occupied, kmq, offsets, weights):
    count_pb = lax.axis_size("pb")
    count_freq = lax.axis_size("freq")
    count_ga = lax.axis_size("ga")
    pair_rows, basis = densities.shape[2:]
    panel_rows = screened.shape[3]
    group = count_freq * count_ga
    pairs = group * pair_rows
    width = basis // CHUNKS
    total_out = OUT_DEV * count_pb * count_freq
    shape = (count_pb, count_freq, count_ga, CHUNKS, width, min(TILE, panel_rows))
    anywhere = pl.BlockSpec(memory_space=pl.ANY)
    scalar = pl.BlockSpec(memory_space=pltpu.SMEM)
    vector = pl.BlockSpec(memory_space=pltpu.VMEM)
    return pl.pallas_call(
        functools.partial(fused_kernel, shape),
        out_shape=jax.ShapeDtypeStruct((2, NS, OUT_DEV), jnp.float32),
        in_specs=[anywhere, anywhere, vector, scalar, scalar, scalar, scalar],
        out_specs=vector,
        scratch_shapes=[
            pltpu.VMEM((CHUNKS, group, 2, pair_rows, width), jnp.bfloat16),
            pltpu.VMEM((CHUNKS, 2, panel_rows, width), jnp.bfloat16),
            pltpu.VMEM((2, 2 * pairs, panel_rows), jnp.float32),
            pltpu.VMEM((2, NB, total_out), jnp.float32),
            pltpu.VMEM((count_pb * group, 2, total_out), jnp.float32),
            pltpu.SemaphoreType.DMA((CHUNKS,)),
            pltpu.SemaphoreType.DMA((CHUNKS,)),
            pltpu.SemaphoreType.DMA((7, CHUNKS)),
            pltpu.SemaphoreType.DMA((7, CHUNKS)),
            pltpu.SemaphoreType.DMA((count_pb * group,)),
            pltpu.SemaphoreType.DMA((count_pb * group,)),
            pltpu.SemaphoreType.REGULAR,
        ],
        compiler_params=pltpu.CompilerParams(
            collective_id=0, has_side_effects=True, vmem_limit_bytes=58 * 2**20
        ),
    )(densities, screened, energies, occupied, kmq, offsets, weights)


def body(densities, screened, *rest):
    chips = lax.axis_size("freq") == 4 and lax.axis_size("ga") == 2
    if chips and densities.shape[2] % 16 == 0 and densities.shape[3] % (CHUNKS * 128) == 0:
        return fused_body(densities, screened, *rest)
    return plain_body(densities, screened, *rest)


def solution(mesh):
    placed = (
        P("pb", None, ("freq", "ga"), None),
        P("pb", "freq", None, "ga", None),
        P(),
        P(),
        P(),
        P(),
        P(),
    )
    return jax.shard_map(
        body, mesh=mesh, in_specs=placed, out_specs=P(None, None, ("pb", "freq")), check_vma=False
    )
```
